16 devices in a mesh: pod: 2 (over y, z), mp: 8 (over x, core).
Axes of the slice: x: 4, y: 2, z: 1, core: 2. Of those that a mesh axis runs over, the one named last changes fastest.
The devices are a block of a 4x4x8 slice.
Arguments:
- d_pool: bfloat16 [32768, 26, 128], P(('pod', 'mp')), parts along dimension 0
- row_ids: int32 [64, 16384, 1], P(('pod', 'mp')), parts along dimension 0
- lengths: int32 [64, 16384], P(('pod', 'mp')), parts along dimension 0
- tables: bfloat16 [64, 16384, 128], P(('pod', 'mp')), parts along dimension 0
- row_accum: float32 [64, 16384], P(('pod', 'mp')), parts along dimension 0
- learn_rate: float32 [], replicated
Outputs:
- output 1: bfloat16 [64, 16384, 128], P(('pod', 'mp')), parts along dimension 0
- output 2: float32 [64, 16384], P(('pod', 'mp')), parts along dimension 0
There are 2 independent parts. The reference program is written for one: setup_inputs(seed, part) draws one part's arguments, and reference() takes and returns one part's arrays. A program takes and returns all parts, laid end to end along the dimension named above; an argument that names none is the same for every part.
All inputs are finite; a program needn't handle non-finite values.
Results may differ from the reference program's by a relative error of at most 0.001.
Values are sent between devices in bfloat16 or wider.
A program may use at most 768 MiB of HBM per device.

```python
import jax
import jax.numpy as jnp
from jax import lax

TABLES = 26
EMB_DIM = 128
TABLE_ROWS = 16384
MAX_HOT = 1
N_SLOTS = 32
BATCH_ALL = 16384
HOT_SET = 64
EPSILON = 1e-06
HOTNESS_LIST = (3, 2, 1, 2, 6, 1, 1, 1, 1, 7, 3, 8, 1, 6, 9, 5, 1, 1, 1, 12, 100, 27, 10, 3, 1, 1)


def slot_hotness():
    hot_list = [min(HOTNESS_LIST[table_idx], MAX_HOT) if table_idx < TABLES else 0 for table_idx in range(N_SLOTS)]
    return jnp.array(hot_list, dtype=jnp.int32)


def draw_routing(route_key):
    slot_hot = slot_hotness()[:, None]
    key_len, key_pick, key_hot, key_uni = jax.random.split(route_key, 4)
    id_shape = (N_SLOTS, BATCH_ALL, MAX_HOT)
    raw_len = jax.random.randint(key_len, (N_SLOTS, BATCH_ALL), 0, 1 << 20)
    lengths = jnp.where(slot_hot > 0, raw_len % (slot_hot + 1), 0)
    lengths = lengths.at[:, 0].set(slot_hot[:, 0])
    hot_pick = jax.random.randint(key_pick, id_shape, 0, 4)
    hot_ids = jax.random.randint(key_hot, id_shape, 0, HOT_SET) * (TABLE_ROWS // HOT_SET)
    uni_ids = jax.random.randint(key_uni, id_shape, 0, TABLE_ROWS)
    row_ids = jnp.where(hot_pick == 0, hot_ids, uni_ids)
    row_ids = row_ids.at[:, 0, 0].set(TABLE_ROWS - 1)
    row_ids = row_ids.at[:, 1, 0].set(0)
    return row_ids.astype(jnp.int32), lengths.astype(jnp.int32)


def setup_inputs(seed: int = 0, part: int = 0) -> dict:
    seed_key = jax.random.key(seed)
    part_key = jax.random.fold_in(seed_key, part)
    key_grad, key_tab, key_acc, key_route = jax.random.split(part_key, 4)
    d_pool = jax.random.normal(key_grad, (BATCH_ALL, TABLES, EMB_DIM), jnp.float32).astype(jnp.bfloat16)
    row_ids, lengths = draw_routing(key_route)
    tables = jax.random.normal(key_tab, (N_SLOTS, TABLE_ROWS, EMB_DIM), jnp.float32).astype(jnp.bfloat16)
    row_accum = jax.random.uniform(key_acc, (N_SLOTS, TABLE_ROWS), jnp.float32, 0.2, 1.0)
    learn_rate = jax.random.uniform(jax.random.key(seed + 1), (), jnp.float32, 0.5, 1.5)
    return {'d_pool': d_pool, 'row_ids': row_ids, 'lengths': lengths, 'tables': tables, 'row_accum': row_accum, 'learn_rate': learn_rate}


def reference(d_pool, row_ids, lengths, tables, row_accum, learn_rate):
    padded = jnp.pad(d_pool, ((0, 0), (0, N_SLOTS - TABLES), (0, 0)))
    by_slot = jnp.transpose(padded, (1, 0, 2))
    positions = jnp.arange(MAX_HOT)

    def one_slot(packed):
        slot_grad, slot_ids, slot_len, slot_table, slot_accum = packed
        grad_vals = slot_grad.astype(jnp.float32)

        def add_position(row_grad, pos_idx):
            keep_mask = (pos_idx < slot_len)[:, None]
            row_grad = row_grad.at[slot_ids[:, pos_idx]].add(jnp.where(keep_mask, grad_vals, 0.0))
            return row_grad, None

        row_grad, unused_out = lax.scan(add_position, jnp.zeros((TABLE_ROWS, EMB_DIM), jnp.float32), positions)
        new_accum = slot_accum + jnp.mean(row_grad * row_grad, axis=-1)
        row_scale = learn_rate / (jnp.sqrt(new_accum) + EPSILON)
        new_table = (slot_table.astype(jnp.float32) - row_grad * row_scale[:, None]).astype(jnp.bfloat16)
        return new_table, new_accum

    new_tables, new_accum = lax.map(one_slot, (by_slot, row_ids, lengths, tables, row_accum))
    return new_tables, new_accum
```

```python
import jax
import jax.numpy as jnp
from jax import lax
from jax.experimental import pallas as pl
from jax.experimental.pallas import tpu as pltpu
from jax.sharding import PartitionSpec as P


EPSILON = 1e-06
LANES = 128
N_ACC = 4
UNROLL = 16


def scatter_adagrad_kernel(ids_ref, lr_ref, grad_ref, table_ref, accum_ref, *refs):
    new_table_ref, new_accum_ref, grad_f32, *accs = refs[-(N_ACC + 3):]
    step = pl.program_id(0)
    n_blk = grad_f32.shape[0]
    n_rows = table_ref.shape[0]

    @pl.when(step == 0)
    def _():
        def zero(i, carry):
            for acc in accs:
                acc[pl.ds(pl.multiple_of(i * 64, 64), 64), :] = jnp.zeros((64, LANES), jnp.float32)
            return carry

        lax.fori_loop(0, n_rows // 64, zero, 0)

    def widen(i, carry):
        rows = pl.ds(pl.multiple_of(i * 128, 128), 128)
        grad_f32[rows, :] = grad_ref[rows, :].astype(jnp.float32)
        return carry

    lax.fori_loop(0, n_blk // 128, widen, 0)

    def add_rows(i, carry):
        base = i * UNROLL
        for first in range(0, UNROLL, N_ACC):
            rows = [ids_ref[step * n_blk + base + first + k] for k in range(N_ACC)]
            sums = [accs[k][pl.ds(rows[k], 1), :] + grad_f32[pl.ds(base + first + k, 1), :] for k in range(N_ACC)]
            for k in range(N_ACC):
                accs[k][pl.ds(rows[k], 1), :] = sums[k]
        return carry

    lax.fori_loop(0, n_blk // UNROLL, add_rows, 0)

    @pl.when(step == pl.num_programs(0) - 1)
    def _():
        lr = lr_ref[0]
        diag = lax.broadcasted_iota(jnp.int32, (LANES, LANES), 0) == lax.broadcasted_iota(jnp.int32, (LANES, LANES), 1)

        def update(i, carry):
            rows = pl.ds(pl.multiple_of(i * LANES, LANES), LANES)
            grad = accs[0][rows, :]
            for acc in accs[1:]:
                grad = grad + acc[rows, :]
            old = jnp.broadcast_to(accum_ref[pl.ds(i, 1), :], (LANES, LANES))
            col = jnp.sum(grad * grad * (1.0 / LANES) + jnp.where(diag, old, 0.0), axis=1, keepdims=True)
            scale = lr / (jnp.sqrt(col) + EPSILON)
            new_table_ref[rows, :] = (table_ref[rows, :].astype(jnp.float32) - grad * scale).astype(jnp.bfloat16)
            new_accum_ref[pl.ds(i, 1), :] = jnp.sum(jnp.where(diag, col, 0.0), axis=0, keepdims=True)
            return carry

        lax.fori_loop(0, n_rows // LANES, update, 0)


def scatter_adagrad(slot, ids, learn_rate, grads, tables, accum, prev):
    n_src, n_blk, dim = grads.shape
    _, n_rows, _ = tables.shape
    once = pl.Buffered(1)
    grid_spec = pltpu.PrefetchScalarGridSpec(
        num_scalar_prefetch=2,
        grid=(n_src,),
        in_specs=[
            pl.BlockSpec((None, n_blk, dim), lambda s, *_: (s, 0, 0)),
            pl.BlockSpec((None, n_rows, dim), lambda s, *_: (slot, 0, 0), pipeline_mode=once),
            pl.BlockSpec((None, n_rows // LANES, LANES), lambda s, *_: (slot, 0, 0), pipeline_mode=once),
        ]
        + [pl.BlockSpec(memory_space=pl.ANY) for _ in prev],
        out_specs=[
            pl.BlockSpec((None, n_rows, dim), lambda s, *_: (slot, 0, 0), pipeline_mode=once),
            pl.BlockSpec((None, n_rows // LANES, LANES), lambda s, *_: (slot, 0, 0), pipeline_mode=once),
        ],
        scratch_shapes=[pltpu.VMEM((n_blk, dim), jnp.float32)]
        + [pltpu.VMEM((n_rows + 8, dim), jnp.float32) for _ in range(N_ACC)],
    )
    return pl.pallas_call(
        scatter_adagrad_kernel,
        grid_spec=grid_spec,
        out_shape=[jax.ShapeDtypeStruct(tables.shape, tables.dtype), jax.ShapeDtypeStruct(accum.shape, accum.dtype)],
        input_output_aliases={5: 0, 6: 1} if prev else {},
        compiler_params=pltpu.CompilerParams(vmem_limit_bytes=60 * 1024 * 1024),
        cost_estimate=pl.CostEstimate(flops=4_000_000_000, bytes_accessed=16 * 1024 * 1024, transcendentals=0),
        name="scatter_adagrad",
    )(ids, learn_rate, grads, tables, accum, *prev)


def solution(mesh):
    n_group = mesh.shape['mp']
    slot_spec = P(('pod', 'mp'))

    def local_step(d_pool, row_ids, lengths, tables, row_accum, learn_rate):
        n_tab = d_pool.shape[1]
        slots_dev, n_rows, dim = tables.shape
        by_slot = jnp.swapaxes(d_pool, 0, 1)
        padded = jnp.pad(by_slot, ((0, slots_dev * n_group - n_tab), (0, 0), (0, 0)))
        by_owner = padded.reshape(n_group, slots_dev, d_pool.shape[0], dim)
        ids = jnp.where(lengths > 0, row_ids[:, :, 0], n_rows)
        accum = row_accum.reshape(slots_dev, n_rows // LANES, LANES)
        lr = learn_rate.reshape(1)
        recv = []
        for j in range(slots_dev):
            send = by_owner[:, j]
            if recv:
                send, recv[-1] = lax.optimization_barrier((send, recv[-1]))
            recv.append(lax.all_to_all(send, 'mp', 0, 0, tiled=True))
        out = ()
        for j in range(slots_dev):
            out = scatter_adagrad(j, ids[j], lr, recv[j], tables, accum, out)
        return out[0], out[1].reshape(slots_dev, n_rows)

    return jax.shard_map(local_step, mesh=mesh, in_specs=(slot_spec, slot_spec, slot_spec, slot_spec, slot_spec, P()), out_specs=(slot_spec, slot_spec), check_vma=False)
```

```python
import functools

import jax
import jax.numpy as jnp
from jax import lax
from jax.experimental import pallas as pl
from jax.experimental.pallas import tpu as pltpu
from jax.sharding import PartitionSpec as P


EPSILON = 1e-06
LANES = 128
N_ACC = 4
UNROLL = 16
SLOTS_PER_DEVICE = 4
FLAG_ROWS = 8
CAPACITY_SHARES = (9, 12, 16)
MIB = 1024 * 1024


def positions_kernel(lens_ref, out_ref):
    n_group, rows_out, _ = out_ref.shape
    per_group = rows_out - FLAG_ROWS
    n_rows = lens_ref.shape[0]
    slots_dev = n_group and n_rows // (n_group * (per_group // SLOTS_PER_DEVICE))
    blocks = per_group // slots_dev
    valid = (lens_ref[...] > 0).astype(jnp.bfloat16)
    lane_i = lax.broadcasted_iota(jnp.int32, (LANES, LANES), 0)
    lane_j = lax.broadcasted_iota(jnp.int32, (LANES, LANES), 1)
    before = (lane_i < lane_j).astype(jnp.bfloat16)
    inside = jnp.dot(valid, before, preferred_element_type=jnp.float32)
    total = jnp.dot(valid, jnp.ones((LANES, LANES), jnp.bfloat16), preferred_element_type=jnp.float32)
    row_i = lax.broadcasted_iota(jnp.int32, (n_rows, n_rows), 0)
    row_j = lax.broadcasted_iota(jnp.int32, (n_rows, n_rows), 1)
    earlier = ((row_j < row_i) & (row_j // blocks == row_i // blocks)).astype(jnp.bfloat16)
    ahead = jnp.dot(earlier, total.astype(jnp.bfloat16), preferred_element_type=jnp.float32)
    code = ((inside + ahead) * 2.0 + valid.astype(jnp.float32)).astype(jnp.int32)
    largest = jnp.max(ahead + total, axis=0, keepdims=True).astype(jnp.int32)
    for d in range(n_group):
        for j in range(slots_dev):
            first = (j * n_group + d) * blocks
            out_ref[d, j * blocks : (j + 1) * blocks, :] = code[first : first + blocks, :]
        out_ref[d, per_group:, :] = jnp.broadcast_to(largest, (FLAG_ROWS, LANES))


def bag_positions(lengths, n_group):
    slots_dev, batch_all = lengths.shape
    per_group = slots_dev * batch_all // (n_group * LANES)
    return pl.pallas_call(
        positions_kernel,
        out_shape=jax.ShapeDtypeStruct((n_group, per_group + FLAG_ROWS, LANES), jnp.int32),
        name="bag_positions",
    )(lengths.reshape(slots_dev * batch_all // LANES, LANES))


def pack_rows_kernel(slot, n_tab, slots_dev, first_ref, code_ref, grad_ref, out_ref, packed):
    dst = pl.program_id(0)
    blocks = grad_ref.shape[0] // LANES
    cap = out_ref.shape[0]

    @pl.when(dst * slots_dev + slot < n_tab)
    def _():
        code = code_ref[slot * blocks : (slot + 1) * blocks, :]
        pos = code >> 1
        rel = jnp.where((code & 1) == 1, pos - pos[:, :1], -1).astype(jnp.float32)
        target = lax.broadcasted_iota(jnp.int32, (LANES, LANES), 0).astype(jnp.float32)
        for b in range(blocks):
            pick = jnp.where(target == rel[b : b + 1, :], 1.0, 0.0).astype(jnp.bfloat16)
            rows = jnp.dot(pick, grad_ref[b * LANES : (b + 1) * LANES, :], preferred_element_type=jnp.float32)
            first = first_ref[(dst * slots_dev + slot) * blocks + b]
            packed[pl.ds(first, LANES), :] = rows

        def narrow(i, carry):
            rows = pl.ds(pl.multiple_of(i * LANES, LANES), LANES)
            out_ref[rows, :] = packed[rows, :].astype(jnp.bfloat16)
            return carry

        lax.fori_loop(0, cap // LANES, narrow, 0)


def pack_rows(slot, slots_dev, cap, firsts, codes, by_slot):
    n_tab, batch, dim = by_slot.shape
    n_group = codes.shape[0]
    grid_spec = pltpu.PrefetchScalarGridSpec(
        num_scalar_prefetch=1,
        grid=(n_group,),
        in_specs=[
            pl.BlockSpec((None,) + codes.shape[1:], lambda d, *_: (d, 0, 0)),
            pl.BlockSpec((None, batch, dim), lambda d, *_: (jnp.minimum(d * slots_dev + slot, n_tab - 1), 0, 0)),
        ],
        out_specs=pl.BlockSpec((None, cap, dim), lambda d, *_: (d, 0, 0)),
        scratch_shapes=[pltpu.VMEM((cap + LANES, dim), jnp.float32)],
    )
    return pl.pallas_call(
        functools.partial(pack_rows_kernel, slot, n_tab, slots_dev),
        grid_spec=grid_spec,
        out_shape=jax.ShapeDtypeStruct((n_group, cap, dim), by_slot.dtype),
        cost_estimate=pl.CostEstimate(flops=500_000_000, bytes_accessed=8 * MIB, transcendentals=0),
        name="pack_rows",
    )(firsts, codes, by_slot)


def pack_ids_kernel(first_ref, code_ref, ids_ref, out_ref, packed, *, n_rows):
    slot = pl.program_id(0)
    n_group = code_ref.shape[0]
    blocks = ids_ref.shape[0] // n_group
    per_src = out_ref.shape[0] // n_group
    slots_dev = pl.num_programs(0)
    n_high = n_rows // LANES
    target = lax.broadcasted_iota(jnp.int32, (2 * LANES, LANES), 0).astype(jnp.float32)
    part = lax.broadcasted_iota(jnp.int32, (8, LANES), 0)

    def one_source(src, carry):
        packed[...] = jnp.zeros_like(packed)
        for b in range(blocks):
            row = first_ref[(src * slots_dev + slot) * blocks + b] // LANES
            code = code_ref[src, pl.ds(slot * blocks + b, 1), :]
            rel = jnp.where((code & 1) == 1, (code >> 1) - row * LANES, -1).astype(jnp.float32)
            pick = jnp.where(target == rel, 1.0, 0.0).astype(jnp.bfloat16)
            ids = ids_ref[pl.ds(src * blocks + b, 1), :]
            parts = jnp.where(part == 0, n_high - ids // LANES, jnp.where(part == 1, ids % LANES, 0)).astype(jnp.bfloat16)
            moved = lax.dot_general(parts, pick, (((1,), (1,)), ((), ())), preferred_element_type=jnp.float32)
            packed[row] = packed[row] + moved[:, :LANES]
            packed[row + 1] = packed[row + 1] + moved[:, LANES:]
        for r in range(per_src):
            both = packed[r].astype(jnp.int32)
            out_ref[pl.ds(src * per_src + r, 1), :] = (n_high - both[0:1, :]) * LANES + both[1:2, :]
        return carry

    lax.fori_loop(0, n_group, one_source, 0)


def pack_ids(cap, firsts, codes, ids, n_rows):
    slots_dev, batch_all = ids.shape
    n_group = codes.shape[0]
    rows_out = n_group * cap // LANES
    grid_spec = pltpu.PrefetchScalarGridSpec(
        num_scalar_prefetch=1,
        grid=(slots_dev,),
        in_specs=[
            pl.BlockSpec(codes.shape, lambda j, *_: (0, 0, 0)),
            pl.BlockSpec((None, batch_all // LANES, LANES), lambda j, *_: (j, 0, 0)),
        ],
        out_specs=pl.BlockSpec((None, rows_out, LANES), lambda j, *_: (j, 0, 0)),
        scratch_shapes=[pltpu.VMEM((cap // LANES + 2, 8, LANES), jnp.float32)],
    )
    return pl.pallas_call(
        functools.partial(pack_ids_kernel, n_rows=n_rows),
        grid_spec=grid_spec,
        out_shape=jax.ShapeDtypeStruct((slots_dev, rows_out, LANES), jnp.int32),
        cost_estimate=pl.CostEstimate(flops=1_000_000_000, bytes_accessed=MIB, transcendentals=0),
        name="pack_ids",
    )(firsts, codes, ids.reshape(slots_dev, batch_all // LANES, LANES))


def scatter_adagrad_kernel(slot, n_prev, ids_ref, count_ref, lr_ref, grad_ref, table_hbm, accum_ref, *refs):
    prev_refs, refs = refs[:n_prev], refs[n_prev:]
    new_table_hbm, new_accum_ref, grad_f32, table, scale_ref, sems, *accs = refs
    step = pl.program_id(0)
    cap = grad_f32.shape[0]
    n_rows = table.shape[0]
    n_out = sems.shape[0] - 1
    load_table = pltpu.make_async_copy(table_hbm.at[slot], table, sems.at[n_out])

    @pl.when(step == 0)
    def _():
        load_table.start()
        if n_prev:
            new_accum_ref[...] = prev_refs[1][...]

        def zero(i, carry):
            for acc in accs:
                acc[pl.ds(pl.multiple_of(i * 64, 64), 64), :] = jnp.zeros((64, LANES), jnp.float32)
            return carry

        lax.fori_loop(0, n_rows // 64, zero, 0)

    count = count_ref[step]

    def widen(i, carry):
        rows = pl.ds(pl.multiple_of(i * LANES, LANES), LANES)
        grad_f32[rows, :] = grad_ref[rows, :].astype(jnp.float32)
        return carry

    lax.fori_loop(0, (count + LANES - 1) // LANES, widen, 0)

    def add_rows(i, carry):
        base = i * UNROLL
        for first in range(0, UNROLL, N_ACC):
            rows = [ids_ref[step * cap + base + first + k] for k in range(N_ACC)]
            sums = [accs[k][pl.ds(rows[k], 1), :] + grad_f32[pl.ds(base + first + k, 1), :] for k in range(N_ACC)]
            for k in range(N_ACC):
                accs[k][pl.ds(rows[k], 1), :] = sums[k]
        return carry

    lax.fori_loop(0, (count + UNROLL - 1) // UNROLL, add_rows, 0)

    @pl.when(step == pl.num_programs(0) - 1)
    def _():
        lr = lr_ref[0]
        diag = lax.broadcasted_iota(jnp.int32, (LANES, LANES), 0) == lax.broadcasted_iota(jnp.int32, (LANES, LANES), 1)

        def square(i, carry):
            rows = pl.ds(pl.multiple_of(i * LANES, LANES), LANES)
            grad = accs[0][rows, :]
            for acc in accs[1:]:
                grad = grad + acc[rows, :]
            accs[0][rows, :] = grad
            old = jnp.broadcast_to(accum_ref[slot : slot + 1, rows], (LANES, LANES))
            col = jnp.sum(grad * grad * (1.0 / LANES) + jnp.where(diag, old, 0.0), axis=1, keepdims=True)
            row = jnp.sum(jnp.where(diag, col, 0.0), axis=0, keepdims=True)
            new_accum_ref[slot : slot + 1, rows] = row
            scale_ref[pl.ds(i, 1), :] = row
            return carry

        lax.fori_loop(0, n_rows // LANES, square, 0)
        scale_ref[...] = lr / (jnp.sqrt(scale_ref[...]) + EPSILON)
        load_table.wait()
        part = n_rows // n_out

        def store_part(k):
            rows = pl.ds(pl.multiple_of(k * part, part), part)
            return pltpu.make_async_copy(table.at[rows, :], new_table_hbm.at[slot, rows, :], sems.at[k])

        def update_part(k, carry):
            def update(m, carry):
                i = k * (part // LANES) + m
                rows = pl.ds(pl.multiple_of(i * LANES, LANES), LANES)
                scale = jnp.sum(jnp.where(diag, jnp.broadcast_to(scale_ref[pl.ds(i, 1), :], (LANES, LANES)), 0.0), axis=1, keepdims=True)
                table[rows, :] = (table[rows, :].astype(jnp.float32) - accs[0][rows, :] * scale).astype(jnp.bfloat16)
                return carry

            lax.fori_loop(0, part // LANES, update, 0)
            store_part(k).start()
            return carry

        lax.fori_loop(0, n_out, update_part, 0)

        def finish(k, carry):
            store_part(k).wait()
            return carry

        lax.fori_loop(0, n_out, finish, 0)


def scatter_adagrad(slot, ids, counts, learn_rate, grads, tables, accum, prev):
    n_src, cap, dim = grads.shape
    n_rows = tables.shape[1]
    n_out = 8
    whole_accum = pl.BlockSpec(accum.shape, lambda s, *_: (0, 0))
    grid_spec = pltpu.PrefetchScalarGridSpec(
        num_scalar_prefetch=3,
        grid=(n_src,),
        in_specs=[
            pl.BlockSpec((None, cap, dim), lambda s, *_: (s, 0, 0)),
            pl.BlockSpec(memory_space=pl.ANY),
            whole_accum,
        ]
        + ([pl.BlockSpec(memory_space=pl.ANY), whole_accum] if prev else []),
        out_specs=[pl.BlockSpec(memory_space=pl.ANY), whole_accum],
        scratch_shapes=[
            pltpu.VMEM((cap, dim), jnp.float32),
            pltpu.VMEM((n_rows, dim), jnp.bfloat16),
            pltpu.VMEM((n_rows // LANES, LANES), jnp.float32),
            pltpu.SemaphoreType.DMA((n_out + 1,)),
        ]
        + [pltpu.VMEM((n_rows + 8, dim), jnp.float32) for _ in range(N_ACC)],
    )
    return pl.pallas_call(
        functools.partial(scatter_adagrad_kernel, slot, len(prev)),
        grid_spec=grid_spec,
        out_shape=[jax.ShapeDtypeStruct(tables.shape, tables.dtype), jax.ShapeDtypeStruct(accum.shape, accum.dtype)],
        input_output_aliases={6: 0, 7: 1} if prev else {},
        compiler_params=pltpu.CompilerParams(vmem_limit_bytes=52 * MIB),
        cost_estimate=pl.CostEstimate(flops=4_000_000_000, bytes_accessed=16 * MIB, transcendentals=0),
        name="scatter_adagrad",
    )(ids, counts, learn_rate, grads, tables, accum, *prev)


def solution(mesh):
    n_group = mesh.shape['mp']
    slot_spec = P(('pod', 'mp'))

    def packed_step(cap, by_slot, ids, own_codes, codes, tables, accum, lr):
        slots_dev, n_rows, _ = tables.shape
        per_group = codes.shape[1] - FLAG_ROWS
        blocks = per_group // slots_dev
        firsts = (codes[:, :per_group, 0] >> 1).reshape(-1)
        own_firsts = (own_codes[:, :per_group, 0] >> 1).reshape(-1)
        last = own_codes[:, blocks - 1 : per_group : blocks, LANES - 1]
        counts = ((last + 1) >> 1).T
        packed_ids = None
        recv = []
        for j in range(slots_dev):
            send = pack_rows(j, slots_dev, cap, firsts, codes, by_slot)
            if recv:
                send, recv[-1] = lax.optimization_barrier((send, recv[-1]))
            recv.append(lax.all_to_all(send, 'mp', 0, 0, tiled=True))
        packed_ids = pack_ids(cap, own_firsts, own_codes, ids, n_rows).reshape(slots_dev, -1)
        out = ()
        for j in range(slots_dev):
            out = scatter_adagrad(j, packed_ids[j], counts[j], lr, recv[j], tables, accum, out)
        return tuple(out)

    def local_step(d_pool, row_ids, lengths, tables, row_accum, learn_rate):
        batch = d_pool.shape[0]
        by_slot = jnp.swapaxes(d_pool, 0, 1)
        own_codes = bag_positions(lengths, n_group)
        codes = lax.all_to_all(own_codes, 'mp', 0, 0, tiled=True)
        largest = jnp.max(codes[:, -1, 0])
        caps = [batch * share // 16 for share in CAPACITY_SHARES]
        level = sum((largest > cap).astype(jnp.int32) for cap in caps[:-1])
        branches = [functools.partial(packed_step, cap) for cap in caps]
        return lax.switch(level, branches, by_slot, row_ids[:, :, 0], own_codes, codes, tables, row_accum, learn_rate.reshape(1))

    return jax.shard_map(local_step, mesh=mesh, in_specs=(slot_spec, slot_spec, slot_spec, slot_spec, slot_spec, P()), out_specs=(slot_spec, slot_spec), check_vma=False)
```
